32 devices in a mesh: pts: 16 (over z, y, core), cen: 2 (over x).
Axes of the slice: x: 2, y: 2, z: 4, core: 2. Of those that a mesh axis runs over, the one named last changes fastest.
Arguments:
- points: bfloat16 [4096, 256], P('pts'), may hold values from -64 to 64
- centroids: bfloat16 [65536, 256], P('cen'), may hold values from -10 to 10
Outputs:
- updated: float32 [65536, 256], P(('cen', 'pts'))
- log_norm: float32 [4096], P('pts')
The draws below stay inside these ranges and needn't reach their ends.
All inputs are finite; a program needn't handle non-finite values.
Results may differ from the reference program's by a relative error of at most 0.0017.
Values may be sent and summed in bfloat16 or wider, within the bound.
A program may use at most 128 MiB of HBM per device.

```python
import math
import jax
import jax.numpy as jnp
from jax import lax

D = 256
K = 65536
NPTS = 4096


def centroid_table(key):
    table = jnp.clip(jax.random.normal(jax.random.fold_in(key, 11), (K, D), jnp.float32), -6.0, 6.0)
    return table


def draw_centroids(key, part):
    return centroid_table(key).astype(jnp.bfloat16)


def draw_points(key, part):
    values = jnp.clip(jax.random.normal(jax.random.fold_in(key, 21), (NPTS, D), jnp.float32), -6.0, 6.0)
    return values.astype(jnp.bfloat16)


def setup_inputs(seed: int = 0) -> dict:
    keys = jax.random.split(jax.random.key(seed), 3)
    return {
        "points": draw_points(jax.random.fold_in(keys[2], 71), 0),
        "centroids": draw_centroids(jax.random.fold_in(keys[2], 71), 0),
    }


inv_temp = 0.0625
prior_count = 1.0


def reference(points, centroids):
    center_norms = jnp.sum(jnp.square(centroids.astype(jnp.float32)), axis=1)
    block_rows = math.gcd(NPTS, 1024)
    batches = points.reshape(NPTS // block_rows, block_rows, D)

    def one_block(totals, batch_rows):
        weighted, masses = totals
        logits = (2.0 * lax.dot_general(batch_rows, centroids, (((1,), (1,)), ((), ())), preferred_element_type=jnp.float32) - center_norms[None, :]) * inv_temp
        peak = jnp.max(logits, axis=1)
        row_log = peak + jnp.log(jnp.sum(jnp.exp(logits - peak[:, None]), axis=1))
        shares = jnp.exp(logits - row_log[:, None]).astype(jnp.bfloat16)
        weighted = weighted + lax.dot_general(shares, batch_rows, (((0,), (0,)), ((), ())), preferred_element_type=jnp.float32)
        masses = masses + jnp.sum(shares.astype(jnp.float32), axis=0)
        return (weighted, masses), row_log

    start = (jnp.zeros((K, D), jnp.float32), jnp.zeros((K,), jnp.float32))
    (weighted, masses), row_logs = lax.scan(one_block, start, batches)
    updated = (centroids.astype(jnp.float32) + weighted) / (prior_count + masses)[:, None]
    return updated, row_logs.reshape(NPTS)
```

```python
import functools
import math

import jax
import jax.numpy as jnp
from jax import lax
from jax.experimental import pallas as pl
from jax.experimental.pallas import tpu as pltpu
from jax.sharding import PartitionSpec as P

inv_temp = 0.0625
prior_count = 1.0
log2e = math.log2(math.e)
MESH = pl.DeviceIdType.MESH


def kernel(
    G, C, points_ref, table_ref, out_ref, norm_ref,
    pts_all, pts_scaled, table, half_norms, scores, shares,
    peaks, local_log, all_local, every_norm, factors,
    load_sem, send_sem, ring_sem, twin_sem, stat_send, stat_recv, norm_send, norm_recv,
):
    T, D = points_ref.shape
    own = table.shape[0]
    R = G // 2
    far = R // 2
    half = T // 2
    N = G * C
    RB = min(256, own)
    NB = own // RB
    me = lax.axis_index("pts")
    cen = lax.axis_index("cen")
    mine = cen * G + me
    core = me % 2
    chip = me // 2
    turn = chip % 2
    pos = (chip // 2) * (1 - turn) + (R - 1 - chip // 2) * turn

    def tile_at(p, c):
        s = p // far
        return ((1 - s) * 2 * p + s * (2 * (R - 1 - p) + 1)) * 2 + c

    twin = me + 1 - 2 * core
    right = tile_at((pos + 1) % R, core)
    left = tile_at((pos + R - 1) % R, core)

    my_points = pts_all.at[pl.ds(pl.multiple_of(me * T, T), T)]
    load_points = pltpu.make_async_copy(points_ref, my_points, load_sem.at[0])
    load_points.start()
    load_table = pltpu.make_async_copy(
        table_ref.at[pl.ds(pl.multiple_of(me * own, own), own)], table, load_sem.at[1]
    )
    load_table.start()

    barrier = pltpu.get_barrier_semaphore()

    def greet(i, carry):
        @pl.when(i != mine)
        def _():
            pl.semaphore_signal(
                barrier, inc=1, device_id={"pts": i % G, "cen": i // G}, device_id_type=MESH
            )
        return carry

    lax.fori_loop(0, N, greet, 0)
    load_points.wait()
    pl.semaphore_wait(barrier, N - 1)

    def rows_of(t, h):
        return pts_all.at[pl.ds(pl.multiple_of(t * T + h * half, half), half)]

    def from_left(d):
        return tile_at((pos + R - d) % R, core)

    def from_right(d):
        return tile_at((pos + d) % R, core)

    def ring_copy(way, d, h, t):
        return pltpu.make_async_remote_copy(
            src_ref=rows_of(t, h), dst_ref=rows_of(t, h), send_sem=send_sem,
            recv_sem=ring_sem.at[way, d, h],
            device_id={"pts": (right, left)[way], "cen": cen}, device_id_type=MESH,
        )

    def twin_copy(way, d, h, t):
        return pltpu.make_async_remote_copy(
            src_ref=rows_of(t, h), dst_ref=rows_of(t, h), send_sem=send_sem,
            recv_sem=twin_sem.at[way, d, h],
            device_id={"pts": twin, "cen": cen}, device_id_type=MESH,
        )

    for h in range(2):
        ring_copy(0, 1, h, me).start()
        ring_copy(1, 1, 1 - h, me).start()
    for h in range(2):
        twin_copy(0, 0, h, me).start()

    load_table.wait()

    def norms(r, carry):
        rows = pl.ds(pl.multiple_of(r * RB, RB), RB)
        block = table[rows, :].astype(jnp.float32)
        total = jnp.sum(block * block, axis=1, keepdims=True)
        half_norms[rows, :] = jnp.broadcast_to(0.5 * total, (RB, T))
        return carry

    lax.fori_loop(0, NB, norms, 0)

    def process(t):
        cols = pl.ds(pl.multiple_of(t * T, T), T)
        tile = pts_all[cols, :]

        def score(r, top):
            rows = pl.ds(pl.multiple_of(r * RB, RB), RB)
            u = lax.dot_general(
                table[rows, :], tile, (((1,), (1,)), ((), ())),
                preferred_element_type=jnp.float32,
            ) - half_norms[rows, :]
            scores[rows, :] = u
            return jnp.maximum(top, jnp.max(u.reshape(RB // 8, 8, T), axis=0))

        top = lax.fori_loop(
            0, NB, score, jnp.full((8, T), -jnp.inf, jnp.float32), unroll=True
        )
        peak = jnp.max(top, axis=0, keepdims=True)

        def weigh(r, total):
            rows = pl.ds(pl.multiple_of(r * RB, RB), RB)
            e = jnp.exp2((scores[rows, :] - peak) * (2.0 * inv_temp * log2e))
            shares[rows, cols] = e.astype(jnp.bfloat16)
            return total + jnp.sum(e.reshape(RB // 8, 8, T), axis=0)

        total = lax.fori_loop(0, NB, weigh, jnp.zeros((8, T), jnp.float32), unroll=True)
        scaled_peak = peak * (2.0 * inv_temp)
        peaks[t] = scaled_peak
        value = scaled_peak + jnp.log(jnp.sum(total, axis=0, keepdims=True))
        local_log[t] = value

        @pl.when(t == me)
        def _():
            all_local[mine] = value

        def tell(c, carry):
            @pl.when(c * G + t != mine)
            def _():
                pltpu.make_async_remote_copy(
                    src_ref=local_log.at[t], dst_ref=all_local.at[mine],
                    send_sem=stat_send, recv_sem=stat_recv,
                    device_id={"pts": t, "cen": c}, device_id_type=MESH,
                ).start()
            return carry

        lax.fori_loop(0, C, tell, 0)

    other = 1 - 2 * core

    def twin_ready(way, d, t):
        for h in range(2):
            twin_copy(way, d, h, t).wait_recv()

    process(me)

    def step(d, carry):
        a, b = from_left(d), from_right(d)

        def pass_on(h0, h1):
            for way, h, t in ((0, h0, a), (1, h1, b)):
                ring_copy(way, d, h, t).wait_recv()

                @pl.when((d + 1 < far) | (h == way))
                def _():
                    ring_copy(way, d + 1, h, t).start()

                twin_copy(way, d, h, t).start()

        pass_on(0, 1)
        la, lb = from_left(d - 1) + other, from_right(d - 1) + other

        def earlier(k, carry):
            @pl.when(k == 0)
            def _():
                twin_ready(0, d - 1, la)

            @pl.when(k == 1)
            def _():
                twin_ready(1, d - 1, lb)

            process(la * (1 - k) + lb * k)
            return carry

        lax.fori_loop(0, jnp.minimum(d, 2), earlier, 0)
        pass_on(1, 0)

        def now(k, carry):
            process(a * (1 - k) + b * k)
            return carry

        lax.fori_loop(0, 2, now, 0)
        return carry

    lax.fori_loop(1, far, step, 0)

    last = from_left(far)
    for way in range(2):
        ring_copy(way, far, way, last).wait_recv()
        twin_copy(way, far, way, last).start()
    twin_ready(0, far - 1, from_left(far - 1) + other)
    twin_ready(1, far - 1, from_right(far - 1) + other)

    def tail(k, carry):
        @pl.when(k == 3)
        def _():
            for way in range(2):
                twin_copy(way, far, way, last + other).wait_recv()

        t = tile_at((pos + jnp.where(k == 0, R - far + 1, jnp.where(k == 1, far - 1, far))) % R, core)
        process(t + jnp.where(k == 2, 0, other))
        return carry

    lax.fori_loop(0, 4, tail, 0)

    pltpu.make_async_copy(
        all_local.at[pl.ds(0, N - 1)], all_local.at[pl.ds(0, N - 1)], stat_recv
    ).wait()
    logs = all_local[...].reshape(N, T)
    crest = jnp.max(logs, axis=0, keepdims=True)
    log_norm = crest + jnp.log(jnp.sum(jnp.exp(logs - crest), axis=0, keepdims=True))
    every_norm[me] = log_norm
    norm_ref[...] = log_norm

    def publish(i, carry):
        peer = (me + i) % G
        pltpu.make_async_remote_copy(
            src_ref=every_norm.at[me], dst_ref=every_norm.at[me],
            send_sem=norm_send, recv_sem=norm_recv,
            device_id={"pts": peer, "cen": cen}, device_id_type=MESH,
        ).start()
        return carry

    lax.fori_loop(1, G, publish, 0)
    group = every_norm.at[pl.ds(0, G - 1)]
    pltpu.make_async_copy(group, group, norm_recv).wait()

    def scale(t, carry):
        cols = pl.ds(pl.multiple_of(t * T, T), T)
        factor = jnp.exp(peaks[t] - every_norm[t])
        factors[:, cols] = jnp.broadcast_to(factor, (8, T))
        column = jnp.broadcast_to(factor, (8, T)).T[:, :1]
        pts_scaled[cols, :] = (pts_all[cols, :].astype(jnp.float32) * column).astype(jnp.bfloat16)
        return carry

    lax.fori_loop(0, G, scale, 0, unroll=2)

    KC = min(16, G)

    def update(r, carry):
        rows = pl.ds(pl.multiple_of(r * RB, RB), RB)

        def chunk(j, sums):
            weighted, mass = sums
            base = pl.multiple_of(j * KC * T, KC * T)
            weighted += jnp.dot(
                shares[rows, pl.ds(base, KC * T)], pts_scaled[pl.ds(base, KC * T), :],
                preferred_element_type=jnp.float32,
            )
            for k in range(KC):
                cols = pl.ds(pl.multiple_of(base + k * T, T), T)
                mass += jnp.sum(
                    (shares[rows, cols].astype(jnp.float32) * factors[:1, cols]).reshape(RB, T // 128, 128),
                    axis=1,
                )
            return weighted, mass

        start = (jnp.zeros((RB, D), jnp.float32), jnp.zeros((RB, 128), jnp.float32))
        weighted, mass = lax.fori_loop(0, G // KC, chunk, start, unroll=True)
        total = prior_count + jnp.sum(mass, axis=1, keepdims=True)
        out_ref[rows, :] = (table[rows, :].astype(jnp.float32) + weighted) / total
        return carry

    lax.fori_loop(0, NB, update, 0)

    sent = pts_all.at[pl.ds(0, (G - 1) * T)]
    pltpu.make_async_copy(sent, sent, send_sem).wait()
    pltpu.make_async_copy(
        all_local.at[pl.ds(0, N - 1)], all_local.at[pl.ds(0, N - 1)], stat_send
    ).wait()
    pltpu.make_async_copy(group, group, norm_send).wait()


def body(G, C, points, centroids):
    T, D = points.shape
    own = centroids.shape[0] // G
    far = G // 4
    updated, log_norm = pl.pallas_call(
        functools.partial(kernel, G, C),
        out_shape=(
            jax.ShapeDtypeStruct((own, D), jnp.float32),
            jax.ShapeDtypeStruct((1, T), jnp.float32),
        ),
        in_specs=[pl.BlockSpec(memory_space=pl.ANY)] * 2,
        out_specs=(pl.BlockSpec(memory_space=pltpu.VMEM),) * 2,
        scratch_shapes=[
            pltpu.VMEM((G * T, D), jnp.bfloat16),
            pltpu.VMEM((G * T, D), jnp.bfloat16),
            pltpu.VMEM((own, D), jnp.bfloat16),
            pltpu.VMEM((own, T), jnp.float32),
            pltpu.VMEM((own, T), jnp.float32),
            pltpu.VMEM((own, G * T), jnp.bfloat16),
            pltpu.VMEM((G, 1, T), jnp.float32),
            pltpu.VMEM((G, 1, T), jnp.float32),
            pltpu.VMEM((G * C, 1, T), jnp.float32),
            pltpu.VMEM((G, 1, T), jnp.float32),
            pltpu.VMEM((8, G * T), jnp.float32),
            pltpu.SemaphoreType.DMA((2,)),
            pltpu.SemaphoreType.DMA,
            pltpu.SemaphoreType.DMA((2, far + 1, 2)),
            pltpu.SemaphoreType.DMA((2, far + 1, 2)),
            pltpu.SemaphoreType.DMA,
            pltpu.SemaphoreType.DMA,
            pltpu.SemaphoreType.DMA,
            pltpu.SemaphoreType.DMA,
        ],
        compiler_params=pltpu.CompilerParams(
            collective_id=0, has_side_effects=True, vmem_limit_bytes=60 * 1024 * 1024
        ),
    )(points, centroids)
    return updated, log_norm.reshape(T)


def solution(mesh):
    placed = (P("pts", None), P("cen", None))
    return jax.shard_map(
        functools.partial(body, mesh.shape["pts"], mesh.shape["cen"]),
        mesh=mesh,
        in_specs=placed,
        out_specs=(P(("cen", "pts"), None), P("pts")),
        check_vma=False,
    )
```

```python
import functools
import math

import jax
import jax.numpy as jnp
from jax import lax
from jax.experimental import pallas as pl
from jax.experimental.pallas import tpu as pltpu
from jax.sharding import PartitionSpec as P

inv_temp = 0.0625
prior_count = 1.0
log2e = math.log2(math.e)
MESH = pl.DeviceIdType.MESH


def kernel(
    G, C, points_ref, table_ref, out_ref, norm_ref,
    pts_all, pts_scaled, table, half_norms, scores, shares,
    peaks, local_log, all_local, every_norm, factors,
    load_sem, send_sem, ring_sem, twin_sem, stat_send, stat_recv, norm_send, norm_recv,
):
    T, D = points_ref.shape
    own = table.shape[0]
    R = G // 2
    far = R // 2
    half = T // 2
    N = G * C
    RB = min(256, own)
    NB = own // RB
    me = lax.axis_index("pts")
    cen = lax.axis_index("cen")
    mine = cen * G + me
    core = me % 2
    chip = me // 2
    turn = chip % 2
    pos = (chip // 2) * (1 - turn) + (R - 1 - chip // 2) * turn

    def tile_at(p, c):
        s = p // far
        return ((1 - s) * 2 * p + s * (2 * (R - 1 - p) + 1)) * 2 + c

    twin = me + 1 - 2 * core
    right = tile_at((pos + 1) % R, core)
    left = tile_at((pos + R - 1) % R, core)

    my_points = pts_all.at[pl.ds(pl.multiple_of(me * T, T), T)]
    load_points = pltpu.make_async_copy(points_ref, my_points, load_sem.at[0])
    load_points.start()
    load_table = pltpu.make_async_copy(
        table_ref.at[pl.ds(pl.multiple_of(me * own, own), own)], table, load_sem.at[1]
    )
    load_table.start()

    barrier = pltpu.get_barrier_semaphore()

    def greet(i, carry):
        @pl.when(i != mine)
        def _():
            pl.semaphore_signal(
                barrier, inc=1, device_id={"pts": i % G, "cen": i // G}, device_id_type=MESH
            )
        return carry

    lax.fori_loop(0, N, greet, 0)
    load_points.wait()
    pl.semaphore_wait(barrier, N - 1)

    def rows_of(t, h):
        return pts_all.at[pl.ds(pl.multiple_of(t * T + h * half, half), half)]

    def from_left(d):
        return tile_at((pos + R - d) % R, core)

    def from_right(d):
        return tile_at((pos + d) % R, core)

    def ring_copy(way, d, h, t):
        return pltpu.make_async_remote_copy(
            src_ref=rows_of(t, h), dst_ref=rows_of(t, h), send_sem=send_sem,
            recv_sem=ring_sem.at[way, d, h],
            device_id={"pts": (right, left)[way], "cen": cen}, device_id_type=MESH,
        )

    def twin_copy(way, d, h, t):
        return pltpu.make_async_remote_copy(
            src_ref=rows_of(t, h), dst_ref=rows_of(t, h), send_sem=send_sem,
            recv_sem=twin_sem.at[way, d, h],
            device_id={"pts": twin, "cen": cen}, device_id_type=MESH,
        )

    for h in range(2):
        ring_copy(0, 1, h, me).start()
        ring_copy(1, 1, 1 - h, me).start()
    for h in range(2):
        twin_copy(0, 0, h, me).start()

    load_table.wait()

    def norms(r, carry):
        rows = pl.ds(pl.multiple_of(r * RB, RB), RB)
        block = table[rows, :].astype(jnp.float32)
        total = jnp.sum(block * block, axis=1, keepdims=True)
        half_norms[rows, :] = jnp.broadcast_to(0.5 * total, (RB, T))
        return carry

    lax.fori_loop(0, NB, norms, 0)

    def process(t):
        cols = pl.ds(pl.multiple_of(t * T, T), T)
        tile = pts_all[cols, :]

        def score(r, top):
            rows = pl.ds(pl.multiple_of(r * RB, RB), RB)
            u = lax.dot_general(
                table[rows, :], tile, (((1,), (1,)), ((), ())),
                preferred_element_type=jnp.float32,
            ) - half_norms[rows, :]
            scores[rows, :] = u
            return jnp.maximum(top, jnp.max(u.reshape(RB // 8, 8, T), axis=0))

        top = lax.fori_loop(
            0, NB, score, jnp.full((8, T), -jnp.inf, jnp.float32), unroll=True
        )
        peak = jnp.max(top, axis=0, keepdims=True)

        def weigh(r, total):
            rows = pl.ds(pl.multiple_of(r * RB, RB), RB)
            e = jnp.exp2((scores[rows, :] - peak) * (2.0 * inv_temp * log2e))
            shares[rows, cols] = e.astype(jnp.bfloat16)
            return total + jnp.sum(e.reshape(RB // 8, 8, T), axis=0)

        total = lax.fori_loop(0, NB, weigh, jnp.zeros((8, T), jnp.float32), unroll=True)
        scaled_peak = peak * (2.0 * inv_temp)
        peaks[t] = scaled_peak
        value = scaled_peak + jnp.log(jnp.sum(total, axis=0, keepdims=True))
        local_log[t] = value

        @pl.when(t == me)
        def _():
            all_local[mine] = value

        def tell(c, carry):
            @pl.when(c * G + t != mine)
            def _():
                pltpu.make_async_remote_copy(
                    src_ref=local_log.at[t], dst_ref=all_local.at[mine],
                    send_sem=stat_send, recv_sem=stat_recv,
                    device_id={"pts": t, "cen": c}, device_id_type=MESH,
                ).start()
            return carry

        lax.fori_loop(0, C, tell, 0)

    other = 1 - 2 * core

    def twin_ready(way, d, t):
        for h in range(2):
            twin_copy(way, d, h, t).wait_recv()

    process(me)

    def step(d, carry):
        a, b = from_left(d), from_right(d)

        def pass_on(h0, h1):
            for way, h, t in ((0, h0, a), (1, h1, b)):
                ring_copy(way, d, h, t).wait_recv()

                @pl.when((d + 1 < far) | (h == way))
                def _():
                    ring_copy(way, d + 1, h, t).start()

                twin_copy(way, d, h, t).start()

        pass_on(0, 1)
        la, lb = from_left(d - 1) + other, from_right(d - 1) + other

        def earlier(k, carry):
            @pl.when(k == 0)
            def _():
                twin_ready(0, d - 1, la)

            @pl.when(k == 1)
            def _():
                twin_ready(1, d - 1, lb)

            process(la * (1 - k) + lb * k)
            return carry

        lax.fori_loop(0, jnp.minimum(d, 2), earlier, 0)
        pass_on(1, 0)

        def now(k, carry):
            process(a * (1 - k) + b * k)
            return carry

        lax.fori_loop(0, 2, now, 0)
        return carry

    lax.fori_loop(1, far, step, 0)

    last = from_left(far)
    for way in range(2):
        ring_copy(way, far, way, last).wait_recv()
        twin_copy(way, far, way, last).start()
    twin_ready(0, far - 1, from_left(far - 1) + other)
    twin_ready(1, far - 1, from_right(far - 1) + other)

    def tail(k, carry):
        @pl.when(k == 3)
        def _():
            for way in range(2):
                twin_copy(way, far, way, last + other).wait_recv()

        t = tile_at((pos + jnp.where(k == 0, R - far + 1, jnp.where(k == 1, far - 1, far))) % R, core)
        process(t + jnp.where(k == 2, 0, other))
        return carry

    lax.fori_loop(0, 4, tail, 0)

    pltpu.make_async_copy(
        all_local.at[pl.ds(0, N - 1)], all_local.at[pl.ds(0, N - 1)], stat_recv
    ).wait()
    logs = all_local[...].reshape(N, T)
    crest = jnp.max(logs, axis=0, keepdims=True)
    log_norm = crest + jnp.log(jnp.sum(jnp.exp(logs - crest), axis=0, keepdims=True))
    every_norm[me] = log_norm
    norm_ref[...] = log_norm

    def publish(i, carry):
        peer = (me + i) % G
        pltpu.make_async_remote_copy(
            src_ref=every_norm.at[me], dst_ref=every_norm.at[me],
            send_sem=norm_send, recv_sem=norm_recv,
            device_id={"pts": peer, "cen": cen}, device_id_type=MESH,
        ).start()
        return carry

    lax.fori_loop(1, G, publish, 0)
    group = every_norm.at[pl.ds(0, G - 1)]
    pltpu.make_async_copy(group, group, norm_recv).wait()

    def scale(t, carry):
        cols = pl.ds(pl.multiple_of(t * T, T), T)
        factor = jnp.exp(peaks[t] - every_norm[t])
        factors[:, cols] = jnp.broadcast_to(factor, (8, T))
        column = jnp.broadcast_to(factor, (8, T)).T[:, :1]
        pts_scaled[cols, :] = (pts_all[cols, :].astype(jnp.float32) * column).astype(jnp.bfloat16)
        return carry

    lax.fori_loop(0, G, scale, 0, unroll=2)

    KC = min(16, G)

    def update(r, carry):
        rows = pl.ds(pl.multiple_of(r * RB, RB), RB)

        def chunk(j, sums):
            weighted, mass = sums
            base = pl.multiple_of(j * KC * T, KC * T)
            weighted += jnp.dot(
                shares[rows, pl.ds(base, KC * T)], pts_scaled[pl.ds(base, KC * T), :],
                preferred_element_type=jnp.float32,
            )
            for k in range(KC):
                cols = pl.ds(pl.multiple_of(base + k * T, T), T)
                part = shares[rows, cols].astype(jnp.float32) * factors[:1, cols]
                for g in range(T // 128):
                    mass += part[:, g * 128:(g + 1) * 128]
            return weighted, mass

        start = (jnp.zeros((RB, D), jnp.float32), jnp.zeros((RB, 128), jnp.float32))
        weighted, mass = lax.fori_loop(0, G // KC, chunk, start, unroll=True)
        total = prior_count + jnp.sum(mass, axis=1, keepdims=True)
        out_ref[rows, :] = (table[rows, :].astype(jnp.float32) + weighted) / total
        return carry

    lax.fori_loop(0, NB, update, 0)

    sent = pts_all.at[pl.ds(0, (G - 1) * T)]
    pltpu.make_async_copy(sent, sent, send_sem).wait()
    pltpu.make_async_copy(
        all_local.at[pl.ds(0, N - 1)], all_local.at[pl.ds(0, N - 1)], stat_send
    ).wait()
    pltpu.make_async_copy(group, group, norm_send).wait()


def body(G, C, points, centroids):
    T, D = points.shape
    own = centroids.shape[0] // G
    far = G // 4
    updated, log_norm = pl.pallas_call(
        functools.partial(kernel, G, C),
        out_shape=(
            jax.ShapeDtypeStruct((own, D), jnp.float32),
            jax.ShapeDtypeStruct((1, T), jnp.float32),
        ),
        in_specs=[pl.BlockSpec(memory_space=pl.ANY)] * 2,
        out_specs=(pl.BlockSpec(memory_space=pltpu.VMEM),) * 2,
        scratch_shapes=[
            pltpu.VMEM((G * T, D), jnp.bfloat16),
            pltpu.VMEM((G * T, D), jnp.bfloat16),
            pltpu.VMEM((own, D), jnp.bfloat16),
            pltpu.VMEM((own, T), jnp.float32),
            pltpu.VMEM((own, T), jnp.float32),
            pltpu.VMEM((own, G * T), jnp.bfloat16),
            pltpu.VMEM((G, 1, T), jnp.float32),
            pltpu.VMEM((G, 1, T), jnp.float32),
            pltpu.VMEM((G * C, 1, T), jnp.float32),
            pltpu.VMEM((G, 1, T), jnp.float32),
            pltpu.VMEM((8, G * T), jnp.float32),
            pltpu.SemaphoreType.DMA((2,)),
            pltpu.SemaphoreType.DMA,
            pltpu.SemaphoreType.DMA((2, far + 1, 2)),
            pltpu.SemaphoreType.DMA((2, far + 1, 2)),
            pltpu.SemaphoreType.DMA,
            pltpu.SemaphoreType.DMA,
            pltpu.SemaphoreType.DMA,
            pltpu.SemaphoreType.DMA,
        ],
        compiler_params=pltpu.CompilerParams(
            collective_id=0, has_side_effects=True, vmem_limit_bytes=60 * 1024 * 1024
        ),
    )(points, centroids)
    return updated, log_norm.reshape(T)


def solution(mesh):
    placed = (P("pts", None), P("cen", None))
    return jax.shard_map(
        functools.partial(body, mesh.shape["pts"], mesh.shape["cen"]),
        mesh=mesh,
        in_specs=placed,
        out_specs=(P(("cen", "pts"), None), P("pts")),
        check_vma=False,
    )
```

```python
import functools
import math

import jax
import jax.numpy as jnp
from jax import lax
from jax.experimental import pallas as pl
from jax.experimental.pallas import tpu as pltpu
from jax.sharding import PartitionSpec as P

inv_temp = 0.0625
prior_count = 1.0
log2e = math.log2(math.e)
MESH = pl.DeviceIdType.MESH


def kernel(
    G, C, points_ref, table_ref, out_ref, norm_ref,
    pts_all, pts_scaled, table, half_norms, scores, shares,
    peaks, local_log, all_local, every_norm, factors,
    load_sem, send_sem, ring_sem, twin_sem, stat_send, stat_recv, norm_send, norm_recv,
):
    T, D = points_ref.shape
    own = table.shape[0]
    R = G // 2
    far = R // 2
    half = T // 2
    N = G * C
    RB = min(256, own)
    NB = own // RB
    me = lax.axis_index("pts")
    cen = lax.axis_index("cen")
    mine = cen * G + me
    core = me % 2
    chip = me // 2
    turn = chip % 2
    pos = (chip // 2) * (1 - turn) + (R - 1 - chip // 2) * turn

    def tile_at(p, c):
        s = p // far
        return ((1 - s) * 2 * p + s * (2 * (R - 1 - p) + 1)) * 2 + c

    twin = me + 1 - 2 * core
    right = tile_at((pos + 1) % R, core)
    left = tile_at((pos + R - 1) % R, core)

    my_points = pts_all.at[pl.ds(pl.multiple_of(me * T, T), T)]
    load_points = pltpu.make_async_copy(points_ref, my_points, load_sem.at[0])
    load_points.start()
    load_table = pltpu.make_async_copy(
        table_ref.at[pl.ds(pl.multiple_of(me * own, own), own)], table, load_sem.at[1]
    )
    load_table.start()

    barrier = pltpu.get_barrier_semaphore()

    for peer in (right, left, twin):
        pl.semaphore_signal(
            barrier, inc=1, device_id={"pts": peer, "cen": cen}, device_id_type=MESH
        )
    for i in range(1, C):
        pl.semaphore_signal(
            barrier, inc=1, device_id={"pts": me, "cen": (cen + i) % C}, device_id_type=MESH
        )
    load_points.wait()
    pl.semaphore_wait(barrier, 2 + C)

    def rows_of(t, h):
        return pts_all.at[pl.ds(pl.multiple_of(t * T + h * half, half), half)]

    def from_left(d):
        return tile_at((pos + R - d) % R, core)

    def from_right(d):
        return tile_at((pos + d) % R, core)

    def ring_copy(way, d, h, t):
        return pltpu.make_async_remote_copy(
            src_ref=rows_of(t, h), dst_ref=rows_of(t, h), send_sem=send_sem,
            recv_sem=ring_sem.at[way, d, h],
            device_id={"pts": (right, left)[way], "cen": cen}, device_id_type=MESH,
        )

    def twin_copy(way, d, h, t):
        return pltpu.make_async_remote_copy(
            src_ref=rows_of(t, h), dst_ref=rows_of(t, h), send_sem=send_sem,
            recv_sem=twin_sem.at[way, d, h],
            device_id={"pts": twin, "cen": cen}, device_id_type=MESH,
        )

    for h in range(2):
        ring_copy(0, 1, h, me).start()
        ring_copy(1, 1, 1 - h, me).start()
    for h in range(2):
        twin_copy(0, 0, h, me).start()

    load_table.wait()

    def norms(r, carry):
        rows = pl.ds(pl.multiple_of(r * RB, RB), RB)
        block = table[rows, :].astype(jnp.float32)
        total = jnp.sum(block * block, axis=1, keepdims=True)
        half_norms[rows, :] = jnp.broadcast_to(0.5 * total, (RB, T))
        return carry

    lax.fori_loop(0, NB, norms, 0)

    def process(t):
        cols = pl.ds(pl.multiple_of(t * T, T), T)
        tile = pts_all[cols, :]

        def score(r, top):
            rows = pl.ds(pl.multiple_of(r * RB, RB), RB)
            u = lax.dot_general(
                table[rows, :], tile, (((1,), (1,)), ((), ())),
                preferred_element_type=jnp.float32,
            ) - half_norms[rows, :]
            scores[rows, :] = u
            return jnp.maximum(top, jnp.max(u.reshape(RB // 8, 8, T), axis=0))

        top = lax.fori_loop(
            0, NB, score, jnp.full((8, T), -jnp.inf, jnp.float32), unroll=True
        )
        peak = jnp.max(top, axis=0, keepdims=True)

        def weigh(r, total):
            rows = pl.ds(pl.multiple_of(r * RB, RB), RB)
            e = jnp.exp2((scores[rows, :] - peak) * (2.0 * inv_temp * log2e))
            shares[rows, cols] = e.astype(jnp.bfloat16)
            return total + jnp.sum(e.reshape(RB // 8, 8, T), axis=0)

        total = lax.fori_loop(0, NB, weigh, jnp.zeros((8, T), jnp.float32), unroll=True)
        scaled_peak = peak * (2.0 * inv_temp)
        peaks[t] = scaled_peak
        value = scaled_peak + jnp.log(jnp.sum(total, axis=0, keepdims=True))
        local_log[t] = value

        @pl.when(t == me)
        def _():
            all_local[mine] = value

        def tell(c, carry):
            @pl.when(c * G + t != mine)
            def _():
                pltpu.make_async_remote_copy(
                    src_ref=local_log.at[t], dst_ref=all_local.at[mine],
                    send_sem=stat_send, recv_sem=stat_recv,
                    device_id={"pts": t, "cen": c}, device_id_type=MESH,
                ).start()
            return carry

        lax.fori_loop(0, C, tell, 0)

    other = 1 - 2 * core

    def twin_ready(way, d, t):
        for h in range(2):
            twin_copy(way, d, h, t).wait_recv()

    process(me)

    def step(d, carry):
        a, b = from_left(d), from_right(d)

        def pass_on(h0, h1):
            for way, h, t in ((0, h0, a), (1, h1, b)):
                ring_copy(way, d, h, t).wait_recv()

                @pl.when((d + 1 < far) | (h == way))
                def _():
                    ring_copy(way, d + 1, h, t).start()

                twin_copy(way, d, h, t).start()

        pass_on(0, 1)
        la, lb = from_left(d - 1) + other, from_right(d - 1) + other

        def earlier(k, carry):
            @pl.when(k == 0)
            def _():
                twin_ready(0, d - 1, la)

            @pl.when(k == 1)
            def _():
                twin_ready(1, d - 1, lb)

            process(la * (1 - k) + lb * k)
            return carry

        lax.fori_loop(0, jnp.minimum(d, 2), earlier, 0)
        pass_on(1, 0)

        def now(k, carry):
            process(a * (1 - k) + b * k)
            return carry

        lax.fori_loop(0, 2, now, 0)
        return carry

    lax.fori_loop(1, far, step, 0)

    last = from_left(far)
    for way in range(2):
        ring_copy(way, far, way, last).wait_recv()
        twin_copy(way, far, way, last).start()
    twin_ready(0, far - 1, from_left(far - 1) + other)
    twin_ready(1, far - 1, from_right(far - 1) + other)

    def tail(k, carry):
        @pl.when(k == 3)
        def _():
            for way in range(2):
                twin_copy(way, far, way, last + other).wait_recv()

        t = tile_at((pos + jnp.where(k == 0, R - far + 1, jnp.where(k == 1, far - 1, far))) % R, core)
        process(t + jnp.where(k == 2, 0, other))
        return carry

    lax.fori_loop(0, 4, tail, 0)

    pltpu.make_async_copy(
        all_local.at[pl.ds(0, N - 1)], all_local.at[pl.ds(0, N - 1)], stat_recv
    ).wait()
    logs = all_local[...].reshape(N, T)
    crest = jnp.max(logs, axis=0, keepdims=True)
    log_norm = crest + jnp.log(jnp.sum(jnp.exp(logs - crest), axis=0, keepdims=True))
    every_norm[me] = log_norm
    norm_ref[...] = log_norm

    def publish(i, carry):
        peer = (me + i) % G
        pltpu.make_async_remote_copy(
            src_ref=every_norm.at[me], dst_ref=every_norm.at[me],
            send_sem=norm_send, recv_sem=norm_recv,
            device_id={"pts": peer, "cen": cen}, device_id_type=MESH,
        ).start()
        return carry

    lax.fori_loop(1, G, publish, 0)
    group = every_norm.at[pl.ds(0, G - 1)]
    pltpu.make_async_copy(group, group, norm_recv).wait()

    def scale(t, carry):
        cols = pl.ds(pl.multiple_of(t * T, T), T)
        factor = jnp.exp(peaks[t] - every_norm[t])
        factors[:, cols] = jnp.broadcast_to(factor, (8, T))
        column = jnp.broadcast_to(factor, (8, T)).T[:, :1]
        pts_scaled[cols, :] = (pts_all[cols, :].astype(jnp.float32) * column).astype(jnp.bfloat16)
        return carry

    lax.fori_loop(0, G, scale, 0, unroll=2)

    KC = min(16, G)

    def update(r, carry):
        rows = pl.ds(pl.multiple_of(r * RB, RB), RB)

        def chunk(j, sums):
            weighted, mass = sums
            base = pl.multiple_of(j * KC * T, KC * T)
            weighted += jnp.dot(
                shares[rows, pl.ds(base, KC * T)], pts_scaled[pl.ds(base, KC * T), :],
                preferred_element_type=jnp.float32,
            )
            for k in range(KC):
                cols = pl.ds(pl.multiple_of(base + k * T, T), T)
                part = shares[rows, cols].astype(jnp.float32) * factors[:1, cols]
                for g in range(T // 128):
                    mass += part[:, g * 128:(g + 1) * 128]
            return weighted, mass

        start = (jnp.zeros((RB, D), jnp.float32), jnp.zeros((RB, 128), jnp.float32))
        weighted, mass = lax.fori_loop(0, G // KC, chunk, start, unroll=True)
        total = prior_count + jnp.sum(mass, axis=1, keepdims=True)
        out_ref[rows, :] = (table[rows, :].astype(jnp.float32) + weighted) / total
        return carry

    lax.fori_loop(0, NB, update, 0)

    sent = pts_all.at[pl.ds(0, (G - 1) * T)]
    pltpu.make_async_copy(sent, sent, send_sem).wait()
    pltpu.make_async_copy(
        all_local.at[pl.ds(0, N - 1)], all_local.at[pl.ds(0, N - 1)], stat_send
    ).wait()
    pltpu.make_async_copy(group, group, norm_send).wait()


def body(G, C, points, centroids):
    T, D = points.shape
    own = centroids.shape[0] // G
    far = G // 4
    updated, log_norm = pl.pallas_call(
        functools.partial(kernel, G, C),
        out_shape=(
            pltpu.VMEM((own, D), jnp.float32),
            jax.ShapeDtypeStruct((1, T), jnp.float32),
        ),
        in_specs=[pl.BlockSpec(memory_space=pl.ANY)] * 2,
        out_specs=(pl.BlockSpec(memory_space=pltpu.VMEM),) * 2,
        scratch_shapes=[
            pltpu.VMEM((G * T, D), jnp.bfloat16),
            pltpu.VMEM((G * T, D), jnp.bfloat16),
            pltpu.VMEM((own, D), jnp.bfloat16),
            pltpu.VMEM((own, T), jnp.float32),
            pltpu.VMEM((own, T), jnp.float32),
            pltpu.VMEM((own, G * T), jnp.bfloat16),
            pltpu.VMEM((G, 1, T), jnp.float32),
            pltpu.VMEM((G, 1, T), jnp.float32),
            pltpu.VMEM((G * C, 1, T), jnp.float32),
            pltpu.VMEM((G, 1, T), jnp.float32),
            pltpu.VMEM((8, G * T), jnp.float32),
            pltpu.SemaphoreType.DMA((2,)),
            pltpu.SemaphoreType.DMA,
            pltpu.SemaphoreType.DMA((2, far + 1, 2)),
            pltpu.SemaphoreType.DMA((2, far + 1, 2)),
            pltpu.SemaphoreType.DMA,
            pltpu.SemaphoreType.DMA,
            pltpu.SemaphoreType.DMA,
            pltpu.SemaphoreType.DMA,
        ],
        compiler_params=pltpu.CompilerParams(
            collective_id=0, has_side_effects=True, vmem_limit_bytes=60 * 1024 * 1024
        ),
    )(points, centroids)
    return updated, log_norm.reshape(T)


def solution(mesh):
    placed = (P("pts", None), P("cen", None))
    return jax.shard_map(
        functools.partial(body, mesh.shape["pts"], mesh.shape["cen"]),
        mesh=mesh,
        in_specs=placed,
        out_specs=(P(("cen", "pts"), None), P("pts")),
        check_vma=False,
    )
```

```python
import functools
import math

import jax
import jax.numpy as jnp
from jax import lax
from jax.experimental import pallas as pl
from jax.experimental.pallas import tpu as pltpu
from jax.sharding import PartitionSpec as P

inv_temp = 0.0625
prior_count = 1.0
log2e = math.log2(math.e)
MESH = pl.DeviceIdType.MESH


def kernel(
    G, C, points_ref, table_ref, out_ref, norm_ref,
    pts_all, pts_scaled, table, half_norms, scores, shares,
    peaks, local_log, all_local, every_norm, factors,
    load_sem, send_sem, ring_sem, twin_sem, stat_send, stat_recv, norm_send, norm_recv,
):
    T, D = points_ref.shape
    own = table.shape[0]
    R = G // 2
    far = R // 2
    half = T // 2
    N = G * C
    RB = min(256, own)
    NB = own // RB
    me = lax.axis_index("pts")
    cen = lax.axis_index("cen")
    mine = cen * G + me
    core = me % 2
    chip = me // 2
    turn = chip % 2
    pos = (chip // 2) * (1 - turn) + (R - 1 - chip // 2) * turn

    def tile_at(p, c):
        s = p // far
        return ((1 - s) * 2 * p + s * (2 * (R - 1 - p) + 1)) * 2 + c

    twin = me + 1 - 2 * core
    right = tile_at((pos + 1) % R, core)
    left = tile_at((pos + R - 1) % R, core)

    my_points = pts_all.at[pl.ds(pl.multiple_of(me * T, T), T)]
    load_points = pltpu.make_async_copy(points_ref, my_points, load_sem.at[0])
    load_points.start()
    load_table = pltpu.make_async_copy(
        table_ref.at[pl.ds(pl.multiple_of(me * own, own), own)], table, load_sem.at[1]
    )
    load_table.start()

    barrier = pltpu.get_barrier_semaphore()

    for peer in (right, left, twin):
        pl.semaphore_signal(
            barrier, inc=1, device_id={"pts": peer, "cen": cen}, device_id_type=MESH
        )
    for i in range(1, C):
        pl.semaphore_signal(
            barrier, inc=1, device_id={"pts": me, "cen": (cen + i) % C}, device_id_type=MESH
        )
    load_points.wait()
    pl.semaphore_wait(barrier, 2 + C)

    def rows_of(t, h):
        return pts_all.at[pl.ds(pl.multiple_of(t * T + h * half, half), half)]

    def from_left(d):
        return tile_at((pos + R - d) % R, core)

    def from_right(d):
        return tile_at((pos + d) % R, core)

    def ring_copy(way, d, h, t):
        return pltpu.make_async_remote_copy(
            src_ref=rows_of(t, h), dst_ref=rows_of(t, h), send_sem=send_sem,
            recv_sem=ring_sem.at[way, d, h],
            device_id={"pts": (right, left)[way], "cen": cen}, device_id_type=MESH,
        )

    def twin_copy(way, d, h, t):
        return pltpu.make_async_remote_copy(
            src_ref=rows_of(t, h), dst_ref=rows_of(t, h), send_sem=send_sem,
            recv_sem=twin_sem.at[way, d, h],
            device_id={"pts": twin, "cen": cen}, device_id_type=MESH,
        )

    for h in range(2):
        ring_copy(0, 1, h, me).start()
        ring_copy(1, 1, 1 - h, me).start()
    for h in range(2):
        twin_copy(0, 0, h, me).start()

    load_table.wait()

    def norms(r, carry):
        rows = pl.ds(pl.multiple_of(r * RB, RB), RB)
        block = table[rows, :].astype(jnp.float32)
        total = jnp.sum(block * block, axis=1, keepdims=True)
        half_norms[rows, :] = jnp.broadcast_to(0.5 * total, (RB, T))
        return carry

    lax.fori_loop(0, NB, norms, 0)

    def process(t):
        cols = pl.ds(pl.multiple_of(t * T, T), T)
        tile = pts_all[cols, :]

        def score(r, top):
            rows = pl.ds(pl.multiple_of(r * RB, RB), RB)
            u = lax.dot_general(
                table[rows, :], tile, (((1,), (1,)), ((), ())),
                preferred_element_type=jnp.float32,
            ) - half_norms[rows, :]
            scores[rows, :] = u
            return jnp.maximum(top, jnp.max(u.reshape(RB // 8, 8, T), axis=0))

        top = lax.fori_loop(
            0, NB, score, jnp.full((8, T), -jnp.inf, jnp.float32), unroll=True
        )
        peak = jnp.max(top, axis=0, keepdims=True)

        def weigh(r, total):
            rows = pl.ds(pl.multiple_of(r * RB, RB), RB)
            e = jnp.exp2((scores[rows, :] - peak) * (2.0 * inv_temp * log2e))
            shares[rows, cols] = e.astype(jnp.bfloat16)
            return total + jnp.sum(e.reshape(RB // 8, 8, T), axis=0)

        total = lax.fori_loop(0, NB, weigh, jnp.zeros((8, T), jnp.float32), unroll=True)
        scaled_peak = peak * (2.0 * inv_temp)
        peaks[t] = scaled_peak
        value = scaled_peak + jnp.log(jnp.sum(total, axis=0, keepdims=True))
        local_log[t] = value

        @pl.when(t == me)
        def _():
            all_local[mine] = value

        def tell(c, carry):
            @pl.when(c * G + t != mine)
            def _():
                pltpu.make_async_remote_copy(
                    src_ref=local_log.at[t], dst_ref=all_local.at[mine],
                    send_sem=stat_send, recv_sem=stat_recv,
                    device_id={"pts": t, "cen": c}, device_id_type=MESH,
                ).start()
            return carry

        lax.fori_loop(0, C, tell, 0)

    other = 1 - 2 * core

    def twin_ready(way, d, t):
        for h in range(2):
            twin_copy(way, d, h, t).wait_recv()

    process(me)

    def step(d, carry):
        a, b = from_left(d), from_right(d)

        def pass_on(h0, h1):
            for way, h, t in ((0, h0, a), (1, h1, b)):
                ring_copy(way, d, h, t).wait_recv()

                @pl.when((d + 1 < far) | (h == way))
                def _():
                    ring_copy(way, d + 1, h, t).start()

                twin_copy(way, d, h, t).start()

        pass_on(0, 1)
        la, lb = from_left(d - 1) + other, from_right(d - 1) + other

        def earlier(k, carry):
            @pl.when(k == 0)
            def _():
                twin_ready(0, d - 1, la)

            @pl.when(k == 1)
            def _():
                twin_ready(1, d - 1, lb)

            process(la * (1 - k) + lb * k)
            return carry

        lax.fori_loop(0, jnp.minimum(d, 2), earlier, 0)
        pass_on(1, 0)

        def now(k, carry):
            process(a * (1 - k) + b * k)
            return carry

        lax.fori_loop(0, 2, now, 0)
        return carry

    lax.fori_loop(1, far, step, 0)

    last = from_left(far)
    for way in range(2):
        ring_copy(way, far, way, last).wait_recv()
        twin_copy(way, far, way, last).start()
    twin_ready(0, far - 1, from_left(far - 1) + other)
    twin_ready(1, far - 1, from_right(far - 1) + other)

    def tail(k, carry):
        @pl.when(k == 3)
        def _():
            for way in range(2):
                twin_copy(way, far, way, last + other).wait_recv()

        t = tile_at((pos + jnp.where(k == 0, R - far + 1, jnp.where(k == 1, far - 1, far))) % R, core)
        process(t + jnp.where(k == 2, 0, other))
        return carry

    lax.fori_loop(0, 4, tail, 0)

    pltpu.make_async_copy(
        all_local.at[pl.ds(0, N - 1)], all_local.at[pl.ds(0, N - 1)], stat_recv
    ).wait()
    logs = all_local[...].reshape(N, T)
    crest = jnp.max(logs, axis=0, keepdims=True)
    log_norm = crest + jnp.log(jnp.sum(jnp.exp(logs - crest), axis=0, keepdims=True))
    every_norm[me] = log_norm
    norm_ref[...] = log_norm

    def publish(i, carry):
        peer = (me + i) % G
        pltpu.make_async_remote_copy(
            src_ref=every_norm.at[me], dst_ref=every_norm.at[me],
            send_sem=norm_send, recv_sem=norm_recv,
            device_id={"pts": peer, "cen": cen}, device_id_type=MESH,
        ).start()
        return carry

    lax.fori_loop(1, G, publish, 0)
    group = every_norm.at[pl.ds(0, G - 1)]
    pltpu.make_async_copy(group, group, norm_recv).wait()

    def scale(t, carry):
        cols = pl.ds(pl.multiple_of(t * T, T), T)
        factor = jnp.exp(peaks[t] - every_norm[t])
        factors[:, cols] = jnp.broadcast_to(factor, (8, T))
        column = jnp.broadcast_to(factor, (8, T)).T[:, :1]
        pts_scaled[cols, :] = (pts_all[cols, :].astype(jnp.float32) * column).astype(jnp.bfloat16)
        return carry

    lax.fori_loop(0, G, scale, 0, unroll=8)

    KC = min(16, G)

    def update(r, carry):
        rows = pl.ds(pl.multiple_of(r * RB, RB), RB)

        def chunk(j, sums):
            weighted, mass = sums
            base = pl.multiple_of(j * KC * T, KC * T)
            weighted += jnp.dot(
                shares[rows, pl.ds(base, KC * T)], pts_scaled[pl.ds(base, KC * T), :],
                preferred_element_type=jnp.float32,
            )
            for k in range(KC):
                cols = pl.ds(pl.multiple_of(base + k * T, T), T)
                part = shares[rows, cols].astype(jnp.float32) * factors[:1, cols]
                for g in range(T // 128):
                    mass += part[:, g * 128:(g + 1) * 128]
            return weighted, mass

        start = (jnp.zeros((RB, D), jnp.float32), jnp.zeros((RB, 128), jnp.float32))
        weighted, mass = lax.fori_loop(0, G // KC, chunk, start, unroll=True)
        total = prior_count + jnp.sum(mass, axis=1, keepdims=True)
        out_ref[rows, :] = (table[rows, :].astype(jnp.float32) + weighted) / total
        return carry

    lax.fori_loop(0, NB, update, 0, unroll=2 if NB % 2 == 0 else 1)

    sent = pts_all.at[pl.ds(0, (G - 1) * T)]
    pltpu.make_async_copy(sent, sent, send_sem).wait()
    pltpu.make_async_copy(
        all_local.at[pl.ds(0, N - 1)], all_local.at[pl.ds(0, N - 1)], stat_send
    ).wait()
    pltpu.make_async_copy(group, group, norm_send).wait()


def body(G, C, points, centroids):
    T, D = points.shape
    own = centroids.shape[0] // G
    far = G // 4
    updated, log_norm = pl.pallas_call(
        functools.partial(kernel, G, C),
        out_shape=(
            pltpu.VMEM((own, D), jnp.float32),
            jax.ShapeDtypeStruct((1, T), jnp.float32),
        ),
        in_specs=[pl.BlockSpec(memory_space=pl.ANY)] * 2,
        out_specs=(pl.BlockSpec(memory_space=pltpu.VMEM),) * 2,
        scratch_shapes=[
            pltpu.VMEM((G * T, D), jnp.bfloat16),
            pltpu.VMEM((G * T, D), jnp.bfloat16),
            pltpu.VMEM((own, D), jnp.bfloat16),
            pltpu.VMEM((own, T), jnp.float32),
            pltpu.VMEM((own, T), jnp.float32),
            pltpu.VMEM((own, G * T), jnp.bfloat16),
            pltpu.VMEM((G, 1, T), jnp.float32),
            pltpu.VMEM((G, 1, T), jnp.float32),
            pltpu.VMEM((G * C, 1, T), jnp.float32),
            pltpu.VMEM((G, 1, T), jnp.float32),
            pltpu.VMEM((8, G * T), jnp.float32),
            pltpu.SemaphoreType.DMA((2,)),
            pltpu.SemaphoreType.DMA,
            pltpu.SemaphoreType.DMA((2, far + 1, 2)),
            pltpu.SemaphoreType.DMA((2, far + 1, 2)),
            pltpu.SemaphoreType.DMA,
            pltpu.SemaphoreType.DMA,
            pltpu.SemaphoreType.DMA,
            pltpu.SemaphoreType.DMA,
        ],
        compiler_params=pltpu.CompilerParams(
            collective_id=0, has_side_effects=True, vmem_limit_bytes=60 * 1024 * 1024
        ),
    )(points, centroids)
    return updated, log_norm.reshape(T)


def solution(mesh):
    placed = (P("pts", None), P("cen", None))
    return jax.shard_map(
        functools.partial(body, mesh.shape["pts"], mesh.shape["cen"]),
        mesh=mesh,
        in_specs=placed,
        out_specs=(P(("cen", "pts"), None), P("pts")),
        check_vma=False,
    )
```
